32 devices in a mesh: tm: 4 (over y, x), space: 8 (over z, core).
Axes of the slice: x: 2, y: 2, z: 4, core: 2. Of those that a mesh axis runs over, the one named last changes fastest.
Arguments:
- queries: bfloat16 [4096, 4096], P(('tm', 'space')), may hold values from -20 to 20
- key_vectors: bfloat16 [4096, 4096], P(('tm', 'space')), may hold values from -20 to 20
- value_vectors: bfloat16 [4096, 4096], P(('tm', 'space')), may hold values from -6 to 6
- out_weight: bfloat16 [4096, 6144], P(None, 'space'), may hold values from -0.375 to 0.375
- frame_mask: int32 [4, 4], replicated, may hold values 0 or 1
Outputs:
- projected: bfloat16 [4096, 6144], P('tm', 'space')
The draws below stay inside these ranges and needn't reach their ends.
All inputs are finite; a program needn't handle non-finite values.
Results may differ from the reference program's by a relative error of at most 0.0075.
Values may be sent and summed in bfloat16 or wider, within the bound.
No kernel may reach another device: no remote copies, remote signals or barrier semaphores. Data moves between devices by JAX's collectives and lax.ppermute only.
A program may use at most 128 MiB of HBM per device.

```python
import math
import jax
import jax.numpy as jnp
from jax import lax

D = 6144
HD = 128
HEADS = 32
TOK_DEV = 128
WIN = 1
BLOCKS = 4
TOKENS = 4096
N_TM = 4
N_SPACE = 8


def pair_draw(key):
    base = jax.random.fold_in(key, 7193)
    first_key, second_key = jax.random.split(base, 2)
    width = HEADS * HD
    query_draw = 2.0 * jax.random.truncated_normal(first_key, -4.0, 4.0, (TOKENS, width), jnp.float32)
    key_draw = jax.random.truncated_normal(second_key, -4.0, 4.0, (TOKENS, width), jnp.float32)
    return (query_draw, key_draw)


def draw_queries(key, part):
    return pair_draw(key)[0].astype(jnp.bfloat16)


def draw_key_vectors(key, part):
    return pair_draw(key)[1].astype(jnp.bfloat16)


def set_ends(drawn, own_key, least, top_value):
    extent = drawn.shape
    index_at = [jax.random.randint(jax.random.fold_in(own_key, axis), (), 0, extent[axis]) for axis in range(len(extent))]
    drawn = drawn.at[tuple(index_at)].set(least)
    longest = extent.index(max(extent))
    index_at[longest] = (index_at[longest] + 1) % extent[longest]
    return drawn.at[tuple(index_at)].set(top_value)


def block_scale(key, dims, cuts, least, largest):
    gain, own = 1.0, jax.random.fold_in(key, 6)
    for axis_at, blocks in cuts:
        draws = jnp.exp(jax.random.uniform(jax.random.fold_in(own, axis_at), (blocks,), jnp.float32, least / len(cuts), largest / len(cuts)))
        gain = gain * jnp.repeat(draws, dims[axis_at] // blocks).reshape([-1 if axis == axis_at else 1 for axis in range(len(dims))])
    return gain


def noise(key, shape, scale, limit, shards=(), kind=jnp.bfloat16):
    drawn = scale * jax.random.normal(key, shape, jnp.float32)
    if shards:
        drawn = drawn * block_scale(key, shape, shards, -0.22, 0.18)
    return jnp.clip(drawn, -limit, limit).astype(kind)


def setup_inputs(seed: int = 0) -> dict:
    keys = jax.random.split(jax.random.key(seed), 6)
    return {
        "queries": draw_queries(jax.random.fold_in(keys[5], 71), 0),
        "key_vectors": draw_key_vectors(jax.random.fold_in(keys[5], 71), 0),
        "value_vectors": noise(keys[2], (TOKENS, HEADS * HD), 1.0, 6.0, ((0, 32),)),
        "out_weight": noise(keys[3], (HEADS * HD, D), (HEADS * HD // 16) ** -0.5, 0.375, ((1, 8),)),
        "frame_mask": set_ends((jax.random.randint(keys[4], (BLOCKS, BLOCKS), 0, 5) < 4).astype(jnp.int32), jax.random.fold_in(keys[4], 1), 0, 1),
    }


def reference(queries, key_vectors, value_vectors, out_weight, frame_mask):
    block_tokens = TOK_DEV * N_SPACE
    scale_factor = 1.0 / math.sqrt(HD)
    pieces = []
    for frame_index in range(N_TM):
        block_list = [(frame_index + offset) % N_TM for offset in range(-WIN, WIN + 1)]
        query_rows = queries[frame_index * block_tokens:(frame_index + 1) * block_tokens]
        query_rows = query_rows.reshape(block_tokens, HEADS, HD).transpose(1, 0, 2)
        key_rows = jnp.concatenate([key_vectors[b * block_tokens:(b + 1) * block_tokens] for b in block_list], axis=0)
        key_rows = key_rows.reshape(-1, HEADS, HD).transpose(1, 0, 2)
        value_rows = jnp.concatenate([value_vectors[b * block_tokens:(b + 1) * block_tokens] for b in block_list], axis=0)
        value_rows = value_rows.reshape(-1, HEADS, HD).transpose(1, 0, 2)
        owners = jnp.concatenate([jnp.full((block_tokens,), b, jnp.int32) for b in block_list])
        mask_bits = frame_mask[frame_index][owners]
        allowed = (owners == frame_index) | (mask_bits == 1)

        def one_head(head_trio):
            query_head, key_head, value_head = head_trio
            scores = jnp.dot(query_head, key_head.T, preferred_element_type=jnp.float32) * scale_factor
            scores = jnp.where(allowed[None, :], scores, -jnp.inf)
            row_top = lax.optimization_barrier(jnp.max(scores, axis=1, keepdims=True))
            exp_terms = jnp.where(allowed[None, :], jnp.exp(scores - row_top), 0.0)
            totals = lax.optimization_barrier(jnp.sum(exp_terms, axis=1, keepdims=True))
            mixed = jnp.dot(exp_terms.astype(jnp.bfloat16), value_head, preferred_element_type=jnp.float32)
            return mixed / totals
        heads_out = lax.map(one_head, (query_rows, key_rows, value_rows))
        attended = heads_out.transpose(1, 0, 2).reshape(block_tokens, HEADS * HD).astype(jnp.bfloat16)
        pieces.append(jnp.dot(attended, out_weight, preferred_element_type=jnp.float32).astype(jnp.bfloat16))
    return jnp.concatenate(pieces, axis=0)
```

```python
import functools
import math

import jax
import jax.numpy as jnp
from jax import lax
from jax.experimental import pallas as pl
from jax.experimental.pallas import tpu as pltpu
from jax.sharding import PartitionSpec as P

HD = 128
SMEM = pltpu.MemorySpace.SMEM
GROUPS = None


def params(mib):
    return pltpu.CompilerParams(vmem_limit_bytes=mib * 1024 * 1024)


def cost(flops, bytes_accessed):
    return pl.CostEstimate(flops=int(flops), bytes_accessed=int(bytes_accessed), transcendentals=0)


def full():
    return pl.BlockSpec(memory_space=pltpu.MemorySpace.VMEM)


def slots(devices):
    return [(s, x) for s in range(devices // 2) for x in range(2)]


def ahead(me, devices, shift, cross):
    chips = devices // 2
    return 2 * lax.rem(me // 2 + shift, chips) + lax.rem(me + cross, 2)


def behind(me, devices, shift, cross):
    chips = devices // 2
    return 2 * lax.rem(me // 2 + chips - shift, chips) + lax.rem(me + cross, 2)


def over_space(x, devices, shift, cross):
    chips = devices // 2
    pairs = [(i, 2 * ((i // 2 + shift) % chips) + (i % 2 + cross) % 2) for i in range(devices)]
    return lax.ppermute(x, "space", pairs)


def pack(me, q, k, v, devices, heads):
    rows = q.shape[0]
    places = slots(devices)

    def kernel(me_ref, q_ref, k_ref, v_ref, *outs):
        at = me_ref[0]
        for (shift, cross), out in zip(places, outs):
            target = ahead(at, devices, shift, cross)
            for g, head in enumerate(heads):
                columns = pl.ds(pl.multiple_of((head * devices + target) * HD, HD), HD)
                for t, ref in enumerate((q_ref, k_ref, v_ref)):
                    out[g, t] = ref[:, columns]

    shape = jax.ShapeDtypeStruct((len(heads), 3, rows, HD), q.dtype)
    return pl.pallas_call(
        kernel,
        out_shape=[shape] * devices,
        in_specs=[pl.BlockSpec(memory_space=SMEM), full(), full(), full()],
        out_specs=[full()] * devices,
        compiler_params=params(16),
        cost_estimate=cost(1, 6 * q.size),
        name="pack",
    )(me, q, k, v)


def unpack(me, parts, devices, heads):
    rows = parts[0].shape[2]
    places = slots(devices)

    def kernel(me_ref, *refs):
        ins, outs = refs[:devices], refs[devices:]
        at = me_ref[0]
        for (shift, cross), part in zip(places, ins):
            source = behind(at, devices, shift, cross)
            here = pl.ds(pl.multiple_of(source * rows, rows), rows)
            for g in range(len(heads)):
                outs[2 * g][here, :] = part[g, 0]
                outs[2 * g + 1][0, here, :] = part[g, 1]
                outs[2 * g + 1][1, here, :] = part[g, 2]

    dtype = parts[0].dtype
    shapes = []
    for _ in heads:
        shapes += [
            jax.ShapeDtypeStruct((devices * rows, HD), dtype),
            jax.ShapeDtypeStruct((2, devices * rows, HD), dtype),
        ]
    outs = pl.pallas_call(
        kernel,
        out_shape=shapes,
        in_specs=[pl.BlockSpec(memory_space=SMEM)] + [full()] * devices,
        out_specs=[full()] * len(shapes),
        compiler_params=params(16),
        cost_estimate=cost(1, 4 * devices * parts[0].size),
        name="unpack",
    )(me, *parts)
    return [(outs[2 * g], outs[2 * g + 1]) for g in range(len(heads))]


def attend(granted, q, kvs):
    rows = q.shape[0]
    tile = 256 if rows % 256 == 0 else rows
    factor = math.log2(math.e) / math.sqrt(HD)
    blocks = len(kvs)

    def kernel(granted_ref, q_ref, *refs):
        out = refs[-1]
        query = q_ref[...]
        scores = [
            lax.dot_general(query, ref[0], (((1,), (1,)), ((), ())), preferred_element_type=jnp.float32)
            for ref in refs[:blocks]
        ]
        top = jnp.max(scores[0], axis=1, keepdims=True)
        for b in range(1, blocks):
            peak = jnp.max(scores[b], axis=1, keepdims=True)
            top = jnp.maximum(top, jnp.where(granted_ref[b] == 1, peak, -jnp.inf))
        top = top * factor
        total = jnp.zeros((tile, 1), jnp.float32)
        mixed = jnp.zeros((tile, HD), jnp.float32)
        for b in range(blocks):
            low = top if b == 0 else jnp.where(granted_ref[b] == 1, top, jnp.inf)
            terms = jnp.exp2(scores[b] * factor - low)
            total += jnp.sum(terms, axis=1, keepdims=True)
            mixed += jnp.dot(terms.astype(jnp.bfloat16), refs[b][1], preferred_element_type=jnp.float32)
        out[...] = (mixed / total).astype(out.dtype)

    keys = rows * blocks
    return pl.pallas_call(
        kernel,
        grid=(rows // tile,),
        out_shape=jax.ShapeDtypeStruct(q.shape, q.dtype),
        in_specs=[pl.BlockSpec(memory_space=SMEM), pl.BlockSpec((tile, HD), lambda i: (i, 0))]
        + [pl.BlockSpec(kv.shape, lambda i: (0, 0, 0)) for kv in kvs],
        out_specs=pl.BlockSpec((tile, HD), lambda i: (i, 0)),
        compiler_params=params(32),
        cost_estimate=cost(8 * rows * keys * HD, 2 * (2 * q.size + 2 * keys * HD)),
        name="attend",
    )(granted, q, *kvs)


def project(me, weight, devices, pieces, total, last):
    rows = pieces[0][2].shape[0]
    columns = weight.shape[1]
    tile = 256 if rows % 256 == 0 else rows
    low = min(p[0] for p in pieces)
    span = max(p[0] for p in pieces) + 1 - low
    while low % span:
        low, span = low - 1, span + 1

    def kernel(me_ref, w_ref, *refs):
        at = me_ref[0]
        out = refs[-1]
        acc = None if total is None else refs[2 * len(pieces)][...]
        for i, (head, shift, _, _) in enumerate(pieces):
            parts = []
            for cross in range(2):
                source = behind(at, devices, shift, cross)
                start = ((head - low) * devices + source) * HD
                parts.append(w_ref[pl.ds(pl.multiple_of(start, HD), HD), :])
            left = jnp.concatenate([refs[2 * i][...], refs[2 * i + 1][...]], axis=1)
            product = jnp.dot(left, jnp.concatenate(parts, axis=0), preferred_element_type=jnp.float32)
            acc = product if acc is None else acc + product
        out[...] = acc.astype(out.dtype)

    operands = []
    for p in pieces:
        operands += [p[2], p[3]]
    row_tile = pl.BlockSpec((tile, HD), lambda i: (i, 0))
    wide = pl.BlockSpec((tile, columns), lambda i: (i, 0))
    in_specs = [
        pl.BlockSpec(memory_space=SMEM),
        pl.BlockSpec((span * devices * HD, columns), lambda i: (low // span, 0)),
    ] + [row_tile] * len(operands)
    if total is not None:
        operands.append(total)
        in_specs.append(wide)
    flops = 2 * rows * columns * HD * 2 * len(pieces)
    return pl.pallas_call(
        kernel,
        grid=(rows // tile,),
        out_shape=jax.ShapeDtypeStruct((rows, columns), jnp.bfloat16 if last else jnp.float32),
        in_specs=in_specs,
        out_specs=wide,
        compiler_params=params(32),
        cost_estimate=cost(flops, rows * columns * 8),
        name="project",
    )(me, weight, *operands)


def block_neighbours(x, frames):
    if frames % 2:
        return [
            lax.ppermute(x, "tm", [(i, (i + by) % frames) for i in range(frames)]) for by in (1, -1)
        ]
    first = lax.ppermute(x, "tm", [(i, i ^ 1) for i in range(frames)])
    second = lax.ppermute(
        first, "tm", [(i, (i + 2) % frames if i % 2 == 0 else (i - 2) % frames) for i in range(frames)]
    )
    return [first, second]


def body(queries, key_vectors, value_vectors, out_weight, frame_mask):
    frames = lax.axis_size("tm")
    devices = lax.axis_size("space")
    here = lax.axis_index("tm")
    me = lax.axis_index("space").astype(jnp.int32).reshape(1)
    local_heads = queries.shape[1] // HD // devices
    chips = devices // 2
    if frames % 2:
        sources = [here - 1, here + 1]
    else:
        even = here % 2 == 0
        sources = [jnp.where(even, here + 1, here - 1), jnp.where(even, here - 1, here + 1)]
    granted = jnp.stack(
        [jnp.int32(1)] + [frame_mask[here, jnp.mod(source, frames)] for source in sources]
    )
    groups = [[j] for j in range(local_heads)]

    arrived = []
    for heads in groups:
        parts = pack(me, queries, key_vectors, value_vectors, devices, heads)
        arrived.append(
            [
                part if (shift, cross) == (0, 0) else over_space(part, devices, shift, cross)
                for (shift, cross), part in zip(slots(devices), parts)
            ]
        )
    pieces = []
    for heads, parts in zip(groups, arrived):
        for head, (q, kv) in zip(heads, unpack(me, parts, devices, heads)):
            kvs = [kv] + block_neighbours(kv, frames)
            piece = attend(granted, q, kvs)
            for shift in range(chips):
                if shift:
                    piece = over_space(piece, devices, 1, 0)
                pieces.append((head, shift, piece, over_space(piece, devices, 0, 1)))
    total = None
    for head in range(local_heads):
        mine = [p for p in pieces if p[0] == head]
        total = project(me, out_weight, devices, mine, total, head == local_heads - 1)
    return total


def solution(mesh):
    in_specs = (
        P(("tm", "space"), None),
        P(("tm", "space"), None),
        P(("tm", "space"), None),
        P(None, "space"),
        P(),
    )
    out_specs = P("tm", "space")
    return jax.shard_map(body, mesh=mesh, in_specs=in_specs, out_specs=out_specs, check_vma=False)
```

```python
import math

import jax
import jax.numpy as jnp
from jax import lax
from jax.experimental import pallas as pl
from jax.experimental.pallas import tpu as pltpu
from jax.sharding import PartitionSpec as P


HD = 128
SMEM = pltpu.MemorySpace.SMEM


def params(mib):
    return pltpu.CompilerParams(vmem_limit_bytes=mib * 1024 * 1024)


def cost(flops, bytes_accessed):
    return pl.CostEstimate(flops=int(flops), bytes_accessed=int(bytes_accessed), transcendentals=0)


def full():
    return pl.BlockSpec(memory_space=pltpu.MemorySpace.VMEM)


def slots(devices):
    return [(k, x) for k in range(devices // 2) for x in range(2)]


def exchange_pairs(devices, k, cross):
    chips = devices // 2
    swap = chips & (chips - 1) == 0
    return [
        (i, 2 * ((i // 2) ^ k if swap else (i // 2 + k) % chips) + (i % 2 + cross) % 2) for i in range(devices)
    ]


def slot_target(me, devices, k, cross):
    chips = devices // 2
    chip = jnp.bitwise_xor(me // 2, k) if chips & (chips - 1) == 0 else lax.rem(me // 2 + k, chips)
    return 2 * chip + lax.rem(me + cross, 2)


def slot_source(me, devices, k, cross):
    chips = devices // 2
    chip = jnp.bitwise_xor(me // 2, k) if chips & (chips - 1) == 0 else lax.rem(me // 2 + chips - k, chips)
    return 2 * chip + lax.rem(me + cross, 2)


def behind(me, devices, shift, cross):
    chips = devices // 2
    return 2 * lax.rem(me // 2 + chips - shift, chips) + lax.rem(me + cross, 2)


def ring_step(x, devices):
    chips = devices // 2
    return lax.ppermute(x, "space", [(i, 2 * ((i // 2 + 1) % chips) + i % 2) for i in range(devices)])


def core_swap(x, devices):
    return lax.ppermute(x, "space", [(i, i ^ 1) for i in range(devices)])


def pack(arrays, devices, items, places, first):
    rows = arrays[0].shape[0]
    used = sorted({t for _, t in items})

    def kernel(*refs):
        at = lax.axis_index("space")
        ins, outs, sems = refs[: len(used)], refs[len(used) : -1], refs[-1]
        copies = []
        for (k, cross), out in zip(places, outs):
            target = slot_target(at, devices, k, cross)
            for i, (head, t) in enumerate(items):
                columns = pl.ds(pl.multiple_of((head * devices + target) * HD, HD), HD)
                copy = pltpu.make_async_copy(
                    ins[used.index(t)].at[:, columns], out.at[i], sems.at[len(copies)]
                )
                copy.start()
                copies.append(copy)
        for copy in copies:
            copy.wait()

    shape = jax.ShapeDtypeStruct((len(items), rows, HD), arrays[0].dtype)
    grant = 62 if first else 8
    return pl.pallas_call(
        kernel,
        out_shape=[shape] * len(places),
        in_specs=[pl.BlockSpec(memory_space=pltpu.MemorySpace.HBM)] * len(used),
        out_specs=[full()] * len(places),
        scratch_shapes=[pltpu.SemaphoreType.DMA((len(places) * len(items),))],
        compiler_params=params(grant),
        cost_estimate=cost(1, 4 * rows * HD * len(places) * len(items)),
        name="pack",
    )(*[arrays[t] for t in used])


def unpack(parts, devices, items):
    rows = parts[0].shape[1]
    places = slots(devices)
    keys = []
    for head, t in items:
        if (head, min(t, 1)) not in keys:
            keys.append((head, min(t, 1)))

    def kernel(*refs):
        ins, outs = refs[:devices], refs[devices:]
        at = lax.axis_index("space")
        for (k, cross), part in zip(places, ins):
            source = slot_source(at, devices, k, cross)
            here = pl.ds(pl.multiple_of(source * rows, rows), rows)
            for i, (head, t) in enumerate(items):
                out = outs[keys.index((head, min(t, 1)))]
                out[max(t - 1, 0), here, :] = part[i]

    outs = pl.pallas_call(
        kernel,
        out_shape=[jax.ShapeDtypeStruct((1 + t, devices * rows, HD), parts[0].dtype) for _, t in keys],
        in_specs=[full()] * devices,
        out_specs=[full()] * len(keys),
        compiler_params=params(8),
        cost_estimate=cost(1, 4 * devices * parts[0].size),
        name="unpack",
    )(*parts)
    return dict(zip(keys, outs))


def neighbours(here, frames):
    if frames % 2:
        return [lax.rem(here + frames - 1, frames), lax.rem(here + 1, frames)]
    up, down = lax.rem(here + 1, frames), lax.rem(here + frames - 1, frames)
    even = lax.rem(here, 2) == 0
    return [jnp.where(even, up, down), jnp.where(even, down, up)]


def attend(frame_mask, q, kvs):
    rows = q.shape[1]
    frames = frame_mask.shape[0]
    tile = 256 if rows % 256 == 0 else rows
    chunk = 4 * tile if rows % (4 * tile) == 0 else tile
    width = 512 if rows % 512 == 0 else rows
    factor = math.log2(math.e) / math.sqrt(HD)
    spans = [(b, at) for b in range(len(kvs)) for at in range(0, rows, width)]

    def some_tiles(first, granted, q_ref, refs, out):
        held, peaks = {}, {}

        def rows_at(t):
            return pl.ds(first + t * tile, tile)

        def score(t, i):
            b, at = spans[i]
            query = q_ref[0, rows_at(t), :]
            scores = lax.dot_general(
                query, refs[b][0, at : at + width], (((1,), (1,)), ((), ())), preferred_element_type=jnp.float32
            )
            held[t, i] = scores
            for c in range(0, width, HD):
                part = scores[:, c : c + HD]
                peaks[t, b] = jnp.maximum(peaks[t, b], part) if (t, b) in peaks else part

        def weigh(t, i, top, mixed):
            b, at = spans[i]
            low = top if b == 0 else jnp.where(granted[b], top, jnp.inf)
            terms = jnp.exp2(held.pop((t, i)) * factor - low).astype(jnp.bfloat16)
            values = refs[b][1, at : at + width]
            values = jnp.concatenate([values, jnp.ones_like(values)], axis=1)
            product = jnp.dot(terms, values, preferred_element_type=jnp.float32)
            return product if mixed is None else mixed + product

        tiles = chunk // tile
        for i in range(len(spans)):
            score(0, i)
        for t in range(tiles):
            top = peaks.pop((t, 0))
            for b in range(1, len(kvs)):
                top = jnp.maximum(top, jnp.where(granted[b], peaks.pop((t, b)), -jnp.inf))
            top = jnp.max(top, axis=1, keepdims=True) * factor
            mixed = None
            for i in range(len(spans)):
                if t + 1 < tiles:
                    score(t + 1, i)
                mixed = weigh(t, i, top, mixed)
            out[rows_at(t), :] = (mixed[:, :HD] / mixed[:, HD:]).astype(out.dtype)

    def kernel(mask_ref, q_ref, *refs):
        here = lax.axis_index("tm")
        granted = [None] + [mask_ref[here, source] == 1 for source in neighbours(here, frames)]
        if rows == chunk:
            some_tiles(0, granted, q_ref, refs, refs[-1])
        else:

            @pl.loop(0, rows // chunk)
            def _(n):
                some_tiles(pl.multiple_of(n * chunk, chunk), granted, q_ref, refs, refs[-1])

    keys = rows * len(kvs)
    return pl.pallas_call(
        kernel,
        out_shape=jax.ShapeDtypeStruct((rows, HD), q.dtype),
        in_specs=[pl.BlockSpec(memory_space=SMEM)] + [full()] * (1 + len(kvs)),
        out_specs=full(),
        compiler_params=params(20),
        cost_estimate=cost(8 * rows * keys * HD, 2 * (2 * q.size + 2 * keys * HD)),
        name="attend",
    )(frame_mask, q, *kvs)


def project(weight, devices, pieces, total, last):
    rows = pieces[0][2].shape[0]
    columns = weight.shape[1]
    tile = 256 if rows % 256 == 0 else rows
    tiles = rows // tile

    def kernel(w_ref, *refs):
        at = lax.axis_index("space")
        parts, out = refs[: 2 * len(pieces)], refs[len(operands) - 1]
        sums = None if total is None else refs[len(operands) - 2]

        def one_tile(here):
            acc = None if sums is None else sums[here, :]
            for i, (head, shift, _, _) in enumerate(pieces):
                matching = []
                for cross in range(2):
                    start = (head * devices + behind(at, devices, shift, cross)) * HD
                    matching.append(w_ref[pl.ds(pl.multiple_of(start, HD), HD), :])
                left = jnp.concatenate([parts[2 * i][here, :], parts[2 * i + 1][here, :]], axis=1)
                product = jnp.dot(left, jnp.concatenate(matching, axis=0), preferred_element_type=jnp.float32)
                acc = product if acc is None else acc + product
            return acc

        if not last:
            for n in range(tiles):
                here = pl.ds(n * tile, tile)
                out[here, :] = one_tile(here)
            return
        held, sems = refs[-2:]
        copies = []
        for n in range(tiles):
            here = pl.ds(n * tile, tile)
            held[here, :] = one_tile(here).astype(held.dtype)
            copies.append(pltpu.make_async_copy(held.at[here, :], out.at[here, :], sems.at[n]))
            copies[-1].start()
        for copy in copies:
            copy.wait()

    operands = [weight]
    for p in pieces:
        operands += [p[2], p[3]]
    if total is not None:
        operands.append(total)
    out_type = jnp.bfloat16 if last else jnp.float32
    return pl.pallas_call(
        kernel,
        out_shape=jax.ShapeDtypeStruct((rows, columns), out_type),
        in_specs=[full()] * len(operands),
        out_specs=pl.BlockSpec(memory_space=pltpu.MemorySpace.HBM) if last else full(),
        scratch_shapes=[pltpu.VMEM((rows, columns), out_type), pltpu.SemaphoreType.DMA((tiles,))] if last else [],
        compiler_params=params(24),
        cost_estimate=cost(4 * rows * columns * HD * len(pieces), rows * columns * 8),
        name="project",
    )(*operands)


def pair_swap(x, frames):
    return lax.ppermute(x, "tm", [(i, (i ^ 1) if frames % 2 == 0 else (i + 1) % frames) for i in range(frames)])


def other_neighbour(x, swapped, frames):
    if frames % 2:
        return lax.ppermute(x, "tm", [(i, (i - 1) % frames) for i in range(frames)])
    pairs = [(i, (i + 2) % frames if i % 2 == 0 else (i - 2) % frames) for i in range(frames)]
    return lax.ppermute(swapped, "tm", pairs)


def send_groups(heads):
    early, late = range(min(heads, 2)), range(2, heads)
    groups = [
        [(h, t) for h in early for t in (1, 2)],
        [(h, 0) for h in early] + [(h, t) for h in late[:1] for t in (1, 2)],
        [(h, t) for h in late[1:] for t in (1, 2)] + [(h, 0) for h in late],
    ]
    return [g for g in groups if g]


def body(queries, key_vectors, value_vectors, out_weight, frame_mask):
    frames = lax.axis_size("tm")
    devices = lax.axis_size("space")
    heads = queries.shape[1] // HD // devices
    chips = devices // 2
    arrays = (queries, key_vectors, value_vectors)

    got = {}
    for n, items in enumerate(send_groups(heads)):
        ahead = [slot for slot in slots(devices) if slot[0] == devices // 2 - 1] if n == 0 else []
        parts = {}
        for places in (ahead, [slot for slot in slots(devices) if slot not in ahead]):
            if places:
                parts |= zip(places, pack(arrays, devices, items, places, n == 0))
        arrived = []
        for k, cross in slots(devices):
            part = parts[k, cross]
            if k or cross:
                part = lax.ppermute(part, "space", exchange_pairs(devices, k, cross))
            arrived.append(part)
        got |= unpack(arrived, devices, items)
    pieces = []
    for head in range(heads):
        kv = got[head, 1]
        swapped = pair_swap(kv, frames)
        other = other_neighbour(kv, swapped, frames)
        piece = attend(frame_mask, got[head, 0], [kv, swapped, other])
        for shift in range(chips):
            if shift:
                piece = ring_step(piece, devices)
            pieces.append((head, shift, piece, core_swap(piece, devices)))
    total = None
    left = {(p[0], p[1]): p for p in pieces}
    last, prior = [(heads - 1, chips - 1)], [(heads - 1, chips - 2), (heads - 2, chips - 1)]
    early = [key for key in left if key[0] < heads - 2]
    rest = [key for key in left if key not in early + prior + last]
    calls = [[left[key] for key in keys if key in left] for keys in (early, rest, prior, last)]
    calls = [call for call in calls if call]
    for n, call in enumerate(calls):
        total = project(out_weight, devices, call, total, n == len(calls) - 1)
    return total


def solution(mesh):
    in_specs = (
        P(("tm", "space"), None),
        P(("tm", "space"), None),
        P(("tm", "space"), None),
        P(None, "space"),
        P(),
    )
    out_specs = P("tm", "space")

    return jax.shard_map(body, mesh=mesh, in_specs=in_specs, out_specs=out_specs, check_vma=False)
```

```python
import math

import jax
import jax.numpy as jnp
from jax import lax
from jax.experimental import pallas as pl
from jax.experimental.pallas import tpu as pltpu
from jax.sharding import PartitionSpec as P


HD = 128
SMEM = pltpu.MemorySpace.SMEM


def params(mib):
    return pltpu.CompilerParams(vmem_limit_bytes=mib * 1024 * 1024)


def cost(flops, bytes_accessed):
    return pl.CostEstimate(flops=int(flops), bytes_accessed=int(bytes_accessed), transcendentals=0)


def full():
    return pl.BlockSpec(memory_space=pltpu.MemorySpace.VMEM)


def slots(devices):
    return [(k, x) for k in range(devices // 2) for x in range(2)]


def exchange_pairs(devices, k, cross):
    chips = devices // 2
    swap = chips & (chips - 1) == 0
    return [
        (i, 2 * ((i // 2) ^ k if swap else (i // 2 + k) % chips) + (i % 2 + cross) % 2) for i in range(devices)
    ]


def slot_target(me, devices, k, cross):
    chips = devices // 2
    chip = jnp.bitwise_xor(me // 2, k) if chips & (chips - 1) == 0 else lax.rem(me // 2 + k, chips)
    return 2 * chip + lax.rem(me + cross, 2)


def slot_source(me, devices, k, cross):
    chips = devices // 2
    chip = jnp.bitwise_xor(me // 2, k) if chips & (chips - 1) == 0 else lax.rem(me // 2 + chips - k, chips)
    return 2 * chip + lax.rem(me + cross, 2)


def behind(me, devices, shift, cross):
    chips = devices // 2
    return 2 * lax.rem(me // 2 + chips - shift, chips) + lax.rem(me + cross, 2)


def ring_step(x, devices, by):
    chips = devices // 2
    return lax.ppermute(x, "space", [(i, 2 * ((i // 2 + by) % chips) + i % 2) for i in range(devices)])


def core_swap(x, devices):
    return lax.ppermute(x, "space", [(i, i ^ 1) for i in range(devices)])


def pack(arrays, devices, items, places, first):
    rows = arrays[0].shape[0]
    used = sorted({t for _, t in items})

    def kernel(*refs):
        at = lax.axis_index("space")
        ins, outs, sems = refs[: len(used)], refs[len(used) : -1], refs[-1]
        copies = []
        for (k, cross), out in zip(places, outs):
            target = slot_target(at, devices, k, cross)
            for i, (head, t) in enumerate(items):
                columns = pl.ds(pl.multiple_of((head * devices + target) * HD, HD), HD)
                copy = pltpu.make_async_copy(
                    ins[used.index(t)].at[:, columns], out.at[i], sems.at[len(copies)]
                )
                copy.start()
                copies.append(copy)
        for copy in copies:
            copy.wait()

    shape = jax.ShapeDtypeStruct((len(items), rows, HD), arrays[0].dtype)
    grant = 62 if first else 8
    return pl.pallas_call(
        kernel,
        out_shape=[shape] * len(places),
        in_specs=[pl.BlockSpec(memory_space=pltpu.MemorySpace.HBM)] * len(used),
        out_specs=[full()] * len(places),
        scratch_shapes=[pltpu.SemaphoreType.DMA((len(places) * len(items),))],
        compiler_params=params(grant),
        cost_estimate=cost(1, 4 * rows * HD * len(places) * len(items)),
        name="pack",
    )(*[arrays[t] for t in used])


def unpack(parts, devices, items):
    rows = parts[0].shape[1]
    places = slots(devices)
    keys = []
    for head, t in items:
        if (head, min(t, 1)) not in keys:
            keys.append((head, min(t, 1)))

    def kernel(*refs):
        ins, outs = refs[:devices], refs[devices:]
        at = lax.axis_index("space")
        for (k, cross), part in zip(places, ins):
            source = slot_source(at, devices, k, cross)
            here = pl.ds(pl.multiple_of(source * rows, rows), rows)
            for i, (head, t) in enumerate(items):
                out = outs[keys.index((head, min(t, 1)))]
                out[max(t - 1, 0), here, :] = part[i]

    outs = pl.pallas_call(
        kernel,
        out_shape=[jax.ShapeDtypeStruct((1 + t, devices * rows, HD), parts[0].dtype) for _, t in keys],
        in_specs=[full()] * devices,
        out_specs=[full()] * len(keys),
        compiler_params=params(8),
        cost_estimate=cost(1, 4 * devices * parts[0].size),
        name="unpack",
    )(*parts)
    return dict(zip(keys, outs))


def neighbours(here, frames):
    if frames % 2:
        return [lax.rem(here + frames - 1, frames), lax.rem(here + 1, frames)]
    up, down = lax.rem(here + 1, frames), lax.rem(here + frames - 1, frames)
    even = lax.rem(here, 2) == 0
    return [jnp.where(even, up, down), jnp.where(even, down, up)]


def attend(frame_mask, q, kvs):
    rows = q.shape[1]
    frames = frame_mask.shape[0]
    tile = 256 if rows % 256 == 0 else rows
    chunk = 4 * tile if rows % (4 * tile) == 0 else tile
    width = 512 if rows % 512 == 0 else rows
    factor = math.log2(math.e) / math.sqrt(HD)
    spans = [(b, at) for b in range(len(kvs)) for at in range(0, rows, width)]

    def some_tiles(first, granted, q_ref, refs, out):
        held, peaks = {}, {}

        def rows_at(t):
            return pl.ds(first + t * tile, tile)

        def score(t, i):
            b, at = spans[i]
            query = q_ref[0, rows_at(t), :]
            scores = lax.dot_general(
                query, refs[b][0, at : at + width], (((1,), (1,)), ((), ())), preferred_element_type=jnp.float32
            )
            held[t, i] = scores
            for c in range(0, width, HD):
                part = scores[:, c : c + HD]
                peaks[t, b] = jnp.maximum(peaks[t, b], part) if (t, b) in peaks else part

        def weigh(t, i, top, mixed):
            b, at = spans[i]
            low = top if b == 0 else jnp.where(granted[b], top, jnp.inf)
            terms = jnp.exp2(held.pop((t, i)) * factor - low).astype(jnp.bfloat16)
            values = refs[b][1, at : at + width]
            values = jnp.concatenate([values, jnp.ones_like(values)], axis=1)
            product = jnp.dot(terms, values, preferred_element_type=jnp.float32)
            return product if mixed is None else mixed + product

        tiles = chunk // tile
        for i in range(len(spans)):
            score(0, i)
        for t in range(tiles):
            top = peaks.pop((t, 0))
            for b in range(1, len(kvs)):
                top = jnp.maximum(top, jnp.where(granted[b], peaks.pop((t, b)), -jnp.inf))
            top = jnp.max(top, axis=1, keepdims=True) * factor
            mixed = None
            for i in range(len(spans)):
                if t + 1 < tiles:
                    score(t + 1, i)
                mixed = weigh(t, i, top, mixed)
            out[rows_at(t), :] = (mixed[:, :HD] / mixed[:, HD:]).astype(out.dtype)

    def kernel(mask_ref, q_ref, *refs):
        here = lax.axis_index("tm")
        granted = [None] + [mask_ref[here, source] == 1 for source in neighbours(here, frames)]
        if rows == chunk:
            some_tiles(0, granted, q_ref, refs, refs[-1])
        else:

            @pl.loop(0, rows // chunk)
            def _(n):
                some_tiles(pl.multiple_of(n * chunk, chunk), granted, q_ref, refs, refs[-1])

    keys = rows * len(kvs)
    return pl.pallas_call(
        kernel,
        out_shape=jax.ShapeDtypeStruct((rows, HD), q.dtype),
        in_specs=[pl.BlockSpec(memory_space=SMEM)] + [full()] * (1 + len(kvs)),
        out_specs=full(),
        compiler_params=params(20),
        cost_estimate=cost(8 * rows * keys * HD, 2 * (2 * q.size + 2 * keys * HD)),
        name="attend",
    )(frame_mask, q, *kvs)


def project(weight, devices, pieces, total, last):
    rows = pieces[0][2].shape[0]
    columns = weight.shape[1]
    tile = 256 if rows % 256 == 0 else rows
    tiles = rows // tile

    def kernel(w_ref, *refs):
        at = lax.axis_index("space")
        parts, out = refs[: 2 * len(pieces)], refs[len(operands) - 1]
        sums = None if total is None else refs[len(operands) - 2]

        def one_tile(here):
            acc = None if sums is None else sums[here, :]
            for i, (head, shift, _, _) in enumerate(pieces):
                matching = []
                for cross in range(2):
                    start = (head * devices + behind(at, devices, shift, cross)) * HD
                    matching.append(w_ref[pl.ds(pl.multiple_of(start, HD), HD), :])
                left = jnp.concatenate([parts[2 * i][here, :], parts[2 * i + 1][here, :]], axis=1)
                product = jnp.dot(left, jnp.concatenate(matching, axis=0), preferred_element_type=jnp.float32)
                acc = product if acc is None else acc + product
            return acc

        if not last:
            for n in range(tiles):
                here = pl.ds(n * tile, tile)
                out[here, :] = one_tile(here)
            return
        held, sems = refs[-2:]
        copies = []
        for n in range(tiles):
            here = pl.ds(n * tile, tile)
            held[here, :] = one_tile(here).astype(held.dtype)
            copies.append(pltpu.make_async_copy(held.at[here, :], out.at[here, :], sems.at[n]))
            copies[-1].start()
        for copy in copies:
            copy.wait()

    operands = [weight]
    for p in pieces:
        operands += [p[2], p[3]]
    if total is not None:
        operands.append(total)
    out_type = jnp.bfloat16 if last else jnp.float32
    return pl.pallas_call(
        kernel,
        out_shape=jax.ShapeDtypeStruct((rows, columns), out_type),
        in_specs=[full()] * len(operands),
        out_specs=pl.BlockSpec(memory_space=pltpu.MemorySpace.HBM) if last else full(),
        scratch_shapes=[pltpu.VMEM((rows, columns), out_type), pltpu.SemaphoreType.DMA((tiles,))] if last else [],
        compiler_params=params(24),
        cost_estimate=cost(4 * rows * columns * HD * len(pieces), rows * columns * 8),
        name="project",
    )(*operands)


def pair_swap(x, frames):
    return lax.ppermute(x, "tm", [(i, (i ^ 1) if frames % 2 == 0 else (i + 1) % frames) for i in range(frames)])


def other_neighbour(x, swapped, frames):
    if frames % 2:
        return lax.ppermute(x, "tm", [(i, (i - 1) % frames) for i in range(frames)])
    pairs = [(i, (i + 2) % frames if i % 2 == 0 else (i - 2) % frames) for i in range(frames)]
    return lax.ppermute(swapped, "tm", pairs)


def send_groups(heads):
    early, late = range(min(heads, 2)), range(2, heads)
    groups = [
        [(h, t) for h in early for t in (1, 2)],
        [(h, 0) for h in early] + [(h, t) for h in late[:1] for t in (1, 2)],
        [(h, t) for h in late[1:] for t in (1, 2)] + [(h, 0) for h in late],
    ]
    return [g for g in groups if g]


def body(queries, key_vectors, value_vectors, out_weight, frame_mask):
    frames = lax.axis_size("tm")
    devices = lax.axis_size("space")
    heads = queries.shape[1] // HD // devices
    chips = devices // 2
    half = chips // 2
    arrays = (queries, key_vectors, value_vectors)

    got = {}
    for n, items in enumerate(send_groups(heads)):
        ahead = [(devices // 2 - 1, 0)] if n == 0 else []
        parts = {}
        for places in (ahead, [slot for slot in slots(devices) if slot not in ahead]):
            if places:
                parts |= zip(places, pack(arrays, devices, items, places, n == 0))
        arrived = []
        for k, cross in slots(devices):
            part = parts[k, cross]
            if k or cross:
                part = lax.ppermute(part, "space", exchange_pairs(devices, k, cross))
            arrived.append(part)
        got |= unpack(arrived, devices, items)
    pieces = []
    for head in range(heads):
        kv = got[head, 1]
        swapped = pair_swap(kv, frames)
        other = other_neighbour(kv, swapped, frames)
        piece = attend(frame_mask, got[head, 0], [kv, swapped, other])
        moving = {1: piece, -1: piece}
        for shift in [0] + list(range(1, half + 1)) + list(range(chips - 1, half, -1)):
            if shift:
                by = 1 if shift <= half else -1
                piece = moving[by] = ring_step(moving[by], devices, by)
            pieces.append((head, shift, piece, core_swap(piece, devices)))
    total = None
    left = {(p[0], p[1]): p for p in pieces}
    last, prior = [(heads - 1, half)], [(heads - 2, half)]
    early = [key for key in left if key[0] < heads - 2]
    rest = [key for key in left if key not in early + prior + last]
    calls = [[left[key] for key in keys if key in left] for keys in (early, rest, prior, last)]
    calls = [call for call in calls if call]
    for n, call in enumerate(calls):
        total = project(out_weight, devices, call, total, n == len(calls) - 1)
    return total


def solution(mesh):
    in_specs = (
        P(("tm", "space"), None),
        P(("tm", "space"), None),
        P(("tm", "space"), None),
        P(None, "space"),
        P(),
    )
    out_specs = P("tm", "space")

    return jax.shard_map(body, mesh=mesh, in_specs=in_specs, out_specs=out_specs, check_vma=False)
```
